32 devices in a mesh: chain: 32 (over z, y, x, core).
Axes of the slice: x: 2, y: 2, z: 4, core: 2. Of those that a mesh axis runs over, the one named last changes fastest.
Arguments:
- sections: float32 [32, 2, 4, 2, 128, 128], P('chain'), may hold values from -1.2 to 1.2
- probes: float32 [2, 2, 128, 4096], P(None, None, None, 'chain'), may hold values from -6 to 6
Outputs:
- prefixes: float32 [32, 2, 4, 2, 128, 128], P('chain')
- reflected: float32 [2, 2, 128, 4096], P(None, None, None, 'chain')
- transmitted: float32 [2, 2, 128, 4096], P(None, None, None, 'chain')
The draws below stay inside these ranges and needn't reach their ends.
All inputs are finite; a program needn't handle non-finite values.
Results may differ from the reference program's by a relative error of at most 0.0003.
Values sent between devices are 32-bit elements; how exact they have to be, the bound alone decides.
A program may use at most 128 MiB of HBM per device.

```python
import math
import jax
import jax.numpy as jnp
from jax import lax

P_SIZE = 128
FREQ = 2
INV_STEPS = 9
SECTIONS = 32
PROBES = 4096


def draw_sections(key, part):
    subkeys = jax.random.split(key, 6)
    full_shape = (SECTIONS, FREQ, 4, 2, P_SIZE, P_SIZE)
    refl_scale = (0.04 / (2.0 * P_SIZE)) ** 0.5
    mix_scale = (0.05 / (2.0 * P_SIZE)) ** 0.5
    jitter = jax.random.truncated_normal(subkeys[0], -6.0, 6.0, full_shape, jnp.float32)
    scales = jnp.array([refl_scale, mix_scale, mix_scale, refl_scale], jnp.float32).reshape(1, 1, 4, 1, 1, 1)
    jitter = jitter * scales
    loss_rates = jax.random.uniform(subkeys[1], (SECTIONS, FREQ, P_SIZE), jnp.float32, 0.5, 3.0)
    radius = jnp.sqrt(0.91 - loss_rates / SECTIONS)
    phases = jax.random.uniform(subkeys[2], (SECTIONS, FREQ, P_SIZE), jnp.float32, -math.pi, math.pi)
    unit_matrix = jnp.eye(P_SIZE, dtype=jnp.float32)
    diag_real = (radius * jnp.cos(phases))[..., None] * unit_matrix
    diag_imag = (radius * jnp.sin(phases))[..., None] * unit_matrix
    direct = jnp.stack([diag_real, diag_imag], axis=2)
    vacant = jnp.zeros_like(direct)
    base_blocks = jnp.stack([vacant, direct, direct, vacant], axis=2)
    cavity_start = jax.random.randint(subkeys[3], (), 0, SECTIONS - 1).astype(jnp.int32)
    section_ids = jnp.arange(SECTIONS, dtype=jnp.int32)
    mirror_flag = jnp.logical_or(section_ids == cavity_start, section_ids == cavity_start + 1).astype(jnp.float32)
    left_phase = jax.random.uniform(subkeys[4], (SECTIONS, FREQ, P_SIZE), jnp.float32, -math.pi, math.pi)
    right_phase = jax.random.uniform(subkeys[5], (SECTIONS, FREQ, P_SIZE), jnp.float32, -math.pi, math.pi)
    pass_phase = 0.5 * (left_phase + right_phase + math.pi)
    mirror_refl = 0.85
    mirror_pass = (0.93 - mirror_refl * mirror_refl) ** 0.5

    def diagonal_block(amplitude, angle):
        block_real = (amplitude * jnp.cos(angle))[..., None] * unit_matrix
        block_imag = (amplitude * jnp.sin(angle))[..., None] * unit_matrix
        return jnp.stack([block_real, block_imag], axis=2)
    mirror_left = diagonal_block(mirror_refl, left_phase)
    mirror_right = diagonal_block(mirror_refl, right_phase)
    mirror_through = diagonal_block(mirror_pass, pass_phase)
    mirror_blocks = jnp.stack([mirror_left, mirror_through, mirror_through, mirror_right], axis=2)
    flag_full = mirror_flag.reshape(SECTIONS, 1, 1, 1, 1, 1)
    blocks = flag_full * mirror_blocks + (1.0 - flag_full) * base_blocks
    return blocks + jitter * (1.0 - 0.9 * flag_full)


def steps_of(rng, extent, cuts, smallest, largest):
    def one(dim, blocks):
        steps = jax.random.uniform(jax.random.fold_in(jax.random.fold_in(rng, 6), dim), (blocks,), jnp.float32, smallest / len(cuts), largest / len(cuts))
        return jnp.repeat(jnp.exp(steps), extent[dim] // blocks).reshape((-1,) + (1,) * (len(extent) - dim - 1))

    gain = one(*cuts[0])
    for cut in cuts[1:]:
        gain = gain * one(*cut)
    return gain


def gaussian(key, shape, width, limit, cuts=(), kind=jnp.bfloat16):
    result = width * jax.random.normal(key, shape, jnp.float32)
    if cuts:
        result = result * steps_of(key, shape, cuts, -0.22, 0.18)
    return jnp.clip(result, -limit, limit).astype(kind)


def setup_inputs(seed: int = 0) -> dict:
    key_list = jax.random.split(jax.random.key(seed), 3)
    sections = draw_sections(jax.random.fold_in(key_list[2], 71), 0)
    probes = gaussian(key_list[1], (FREQ, 2, P_SIZE, PROBES), 1.0, 6.0, ((3, 32),), jnp.float32)
    return dict(sections=sections, probes=probes)


precise = lax.Precision.HIGHEST


def complex_product(former, latter):
    former_re = former[..., 0, :, :]
    former_im = former[..., 1, :, :]
    latter_re = latter[..., 0, :, :]
    latter_im = latter[..., 1, :, :]
    real_part = jnp.einsum("...ij,...jk->...ik", former_re, latter_re, precision=precise) - jnp.einsum("...ij,...jk->...ik", former_im, latter_im, precision=precise)
    imag_part = jnp.einsum("...ij,...jk->...ik", former_re, latter_im, precision=precise) + jnp.einsum("...ij,...jk->...ik", former_im, latter_re, precision=precise)
    return jnp.stack([real_part, imag_part], axis=-3)


def unit_like(block):
    vacant = jnp.zeros_like(block[..., 0, :, :])
    diagonal_one = vacant + jnp.eye(block.shape[-1], dtype=block.dtype)
    return jnp.stack([diagonal_one, vacant], axis=-3)


def scattering_identity(matrix):
    unit_block = unit_like(matrix[:, 0])
    vacant = jnp.zeros_like(unit_block)
    return jnp.stack([vacant, unit_block, unit_block, vacant], axis=1)


def redheffer(first, second):
    first_left, first_back, first_fore, first_right = first[:, 0], first[:, 1], first[:, 2], first[:, 3]
    second_left, second_back, second_fore, second_right = second[:, 0], second[:, 1], second[:, 2], second[:, 3]
    unit_block = unit_like(first_left)
    bounce = complex_product(second_left, first_right)
    system = unit_block - bounce
    resolvent = unit_block
    for iteration in range(INV_STEPS):
        resolvent = complex_product(resolvent, 2.0 * unit_block - complex_product(system, resolvent))
    leading = complex_product(first_back, resolvent)
    new_left = first_left + complex_product(leading, complex_product(second_left, first_fore))
    new_back = complex_product(leading, second_back)
    trailing = second_fore + complex_product(complex_product(second_fore, first_right), complex_product(resolvent, second_left))
    new_fore = complex_product(trailing, first_fore)
    new_right = second_right + complex_product(trailing, complex_product(first_right, second_back))
    return jnp.stack([new_left, new_back, new_fore, new_right], axis=1)


def reference(sections, probes):
    def advance(running, section_block):
        combined = redheffer(running, section_block)
        return combined, combined

    initial = scattering_identity(sections[0])
    chain_total, prefixes = lax.scan(advance, initial, sections)
    reflected = complex_product(chain_total[:, 0], probes)
    transmitted = complex_product(chain_total[:, 2], probes)
    return prefixes, reflected, transmitted
```

```python
import functools

import jax
import jax.numpy as jnp
from jax import lax
from jax.experimental import pallas as pl
from jax.experimental.pallas import tpu as pltpu
from jax.sharding import PartitionSpec as P

INV_STEPS = 9
LEFT, BACK, FORE, RIGHT = range(4)
MESH = pl.DeviceIdType.MESH
f32, bf16 = jnp.float32, jnp.bfloat16


def split(x):
    high = x.astype(bf16)
    return high, (x - high.astype(f32)).astype(bf16)


def quarter_turn(block):
    half = block.shape[1] // 2
    return jnp.concatenate([-block[:, half:], block[:, :half]], axis=1)


def embedded(block):
    return split(jnp.concatenate([block, quarter_turn(block)], axis=0))


def product(former, latter):
    rows = former.shape[0]
    high, low = split(former)
    by_high = jnp.dot(jnp.concatenate([high, low], axis=0), latter[0], preferred_element_type=f32)
    by_low = jnp.dot(high, latter[1], preferred_element_type=f32)
    return by_high[:rows] + by_high[rows:] + by_low


def unit(size):
    row = lax.broadcasted_iota(jnp.int32, (size, 2 * size), 0)
    column = lax.broadcasted_iota(jnp.int32, (size, 2 * size), 1)
    return jnp.where(row == column, 1.0, 0.0).astype(f32)


def star(pairs, work, late=None):
    size = work.shape[1] // 2
    for i, (first, second, _) in enumerate(pairs):
        bounce = product(second[LEFT], embedded(first[RIGHT]))
        work[i, :size] = unit(size) + bounce
        work[i, size:] = product(bounce, embedded(bounce))

    def double(_, carry):
        for i in range(len(pairs)):
            both = work[i]
            grown = product(both, embedded(both[size:]))
            work[i, :size] = both[:size] + grown[:size]
            work[i, size:] = grown[size:]
        return carry

    lax.fori_loop(0, INV_STEPS - 2, double, 0)
    if late is not None:
        late()
    for i, (first, second, emit) in enumerate(pairs):
        partial = work[i, :size]
        resolvent = partial + product(partial, embedded(work[i, size:]))
        second_left = second[LEFT]
        fore = embedded(first[FORE])
        back = embedded(second[BACK])
        leading = product(first[BACK], embedded(resolvent))
        inner = product(resolvent, embedded(second_left))
        emit(LEFT, first[LEFT] + product(leading, embedded(product(second_left, fore))))
        through = product(second[FORE], embedded(first[RIGHT]))
        trailing = second[FORE] + product(through, embedded(inner))
        emit(RIGHT, second[RIGHT] + product(trailing, embedded(product(first[RIGHT], back))))
        emit(BACK, product(leading, back))
        emit(FORE, product(trailing, fore))


def kernel(
    n, levels, sections, probes, prefixes, reflected, transmitted,
    arrived, own, stage, before, work, total, leaving,
    swap_sems, stage_send, stage_recv, total_sems, out_send, out_recv,
):
    me = lax.axis_index("chain")
    core = me % 2
    sibling = me + 1 - 2 * core
    size = probes.shape[2]

    def partner(stride):
        return me + stride - 2 * stride * ((me // stride) % 2)

    barrier = pltpu.get_barrier_semaphore()
    for level in range(levels + 1):
        pl.semaphore_signal(barrier, inc=1, device_id=(partner(1 << level),), device_id_type=MESH)
    pl.semaphore_wait(barrier, levels + 1)

    def remote(source, target, send, recv, device):
        return pltpu.make_async_remote_copy(
            src_ref=source, dst_ref=target, send_sem=send, recv_sem=recv, device_id=(device,), device_id_type=MESH
        )

    swap = remote(sections.at[0, 1 - core], arrived, swap_sems.at[0], swap_sems.at[1], sibling)
    swap.start()

    def joined(block):
        return jnp.concatenate([block[0], block[1]], axis=1)

    vacant = jnp.zeros((size, 2 * size), f32)
    for b in range(4):
        own[core, b] = joined(sections[0, core, b])
        before[b] = vacant if b in (LEFT, RIGHT) else unit(size)
    swap.wait()
    for b in range(4):
        own[1 - core, b] = joined(arrived[b])

    def stage_copy(level, stride, block):
        place = stage.at[level, (me // stride) % 2, block]
        return remote(place, place, stage_send.at[level, block], stage_recv.at[level, block], partner(stride))

    def total_copy(k):
        return remote(
            stage.at[levels, 0, (LEFT, FORE)[k]], total.at[k], total_sems.at[0, k], total_sems.at[1, k], sibling
        )

    def emit_stage(level, stride):
        def emit(block, value):
            stage[level, (me // stride) % 2, block] = value

            @pl.when(level < levels)
            def _():
                stage_copy(level, stride, block).start()

            if block in (LEFT, FORE):

                @pl.when(level == levels)
                def _():
                    total_copy((LEFT, FORE).index(block)).start()

        return emit

    def emit_before(block, value):
        before[block] = value

    if levels:
        first_emit = emit_stage(0, 2)
    else:
        first_emit = emit_stage(0, n)
    star([(own.at[0], own.at[1], first_emit)], work)
    pair_slot = (me // 2) % 2 if levels else 0
    for b in range(4):
        own[1, b] = stage[0, pair_slot, b]

    def climb(level, stride):
        lower, upper = stage.at[level, 0], stage.at[level, 1]

        def wait_for(*blocks):
            for block in blocks:
                stage_copy(level, stride, block).wait_recv()

        wait_for(LEFT, RIGHT)
        star([(lower, upper, emit_stage(level + 1, 2 * stride))], work, lambda: wait_for(BACK, FORE))

        @pl.when((me // stride) % 2 == 1)
        def _():
            star([(lower, before, emit_before)], work)

        return 2 * stride

    lax.fori_loop(0, levels, climb, jnp.int32(2))

    def probe(frequency, whole):
        field = embedded(joined(probes[frequency]))
        result = product(whole, field)
        for k, out in enumerate((reflected, transmitted)):
            out[frequency, 0] = result[k * size : (k + 1) * size, :size]
            out[frequency, 1] = result[k * size : (k + 1) * size, size:]

    probe(core, jnp.concatenate([stage[levels, 0, LEFT], stage[levels, 0, FORE]], axis=0))

    def out_copy(block):
        return remote(
            leaving.at[block], prefixes.at[0, core, block], out_send.at[block], out_recv.at[block], sibling
        )

    def emit_away(block, value):
        leaving[block, 0] = value[:, :size]
        leaving[block, 1] = value[:, size:]
        out_copy(block).start()

    def emit_own(block, value):
        prefixes[0, core, block, 0] = value[:, :size]
        prefixes[0, core, block, 1] = value[:, size:]

    star([(before, own.at[1 - core], emit_away), (before, own.at[core], emit_own)], work)

    for k in range(2):
        total_copy(k).wait()
    probe(1 - core, jnp.concatenate([total[0], total[1]], axis=0))

    def drain(level, stride):
        for block in range(4):
            stage_copy(level, stride, block).wait_send()
        return 2 * stride

    lax.fori_loop(0, levels, drain, jnp.int32(2))
    for block in range(4):
        out_copy(block).wait()


def solution(mesh):
    n = mesh.shape["chain"]
    levels = (n // 2 - 1).bit_length()

    def local(sections, probes):
        size = probes.shape[2]
        wide = (size, 2 * size)
        dma = pltpu.SemaphoreType.DMA
        vmem = pl.BlockSpec(memory_space=pltpu.VMEM)
        return pl.pallas_call(
            functools.partial(kernel, n, levels),
            out_shape=tuple(jax.ShapeDtypeStruct(a.shape, f32) for a in (sections, probes, probes)),
            in_specs=[vmem] * 2,
            out_specs=(vmem,) * 3,
            scratch_shapes=[
                pltpu.VMEM(sections.shape[2:], f32),
                pltpu.VMEM((2, 4) + wide, f32),
                pltpu.VMEM((levels + 1, 2, 4) + wide, f32),
                pltpu.VMEM((4,) + wide, f32),
                pltpu.VMEM((2, 2 * size, 2 * size), f32),
                pltpu.VMEM((2,) + wide, f32),
                pltpu.VMEM(sections.shape[2:], f32),
                dma((2,)),
                dma((max(levels, 1), 4)),
                dma((max(levels, 1), 4)),
                dma((2, 2)),
                dma((4,)),
                dma((4,)),
            ],
            compiler_params=pltpu.CompilerParams(
                collective_id=0, has_side_effects=True, vmem_limit_bytes=48 * 1024 * 1024
            ),
        )(sections, probes)

    placed = (P("chain", None, None, None, None, None), P(None, None, None, "chain"))
    return jax.shard_map(
        local, mesh=mesh, in_specs=placed, out_specs=(placed[0], placed[1], placed[1]), check_vma=False
    )
```

```python
import functools

import jax
import jax.numpy as jnp
from jax import lax
from jax.experimental import pallas as pl
from jax.experimental.pallas import tpu as pltpu
from jax.sharding import PartitionSpec as P

INV_STEPS = 9
LEFT, BACK, FORE, RIGHT = range(4)
MESH = pl.DeviceIdType.MESH
f32, bf16 = jnp.float32, jnp.bfloat16


def split(x):
    high = x.astype(bf16)
    return high, (x - high.astype(f32)).astype(bf16)


def quarter_turn(block):
    half = block.shape[1] // 2
    return jnp.concatenate([-block[:, half:], block[:, :half]], axis=1)


def embedded(block):
    return split(jnp.concatenate([block, quarter_turn(block)], axis=0))


def product(former, latter):
    rows = former.shape[0]
    high, low = split(former)
    by_high = jnp.dot(jnp.concatenate([high, low], axis=0), latter[0], preferred_element_type=f32)
    by_low = jnp.dot(high, latter[1], preferred_element_type=f32)
    return by_high[:rows] + by_high[rows:] + by_low


def unit(size):
    row = lax.broadcasted_iota(jnp.int32, (size, 2 * size), 0)
    column = lax.broadcasted_iota(jnp.int32, (size, 2 * size), 1)
    return jnp.where(row == column, 1.0, 0.0).astype(f32)


def star(pairs, work, early=None, middle=None, late=None):
    size = work.shape[1] // 2
    for i, (first, second, _) in enumerate(pairs):
        bounce = product(second[LEFT], embedded(first[RIGHT]))
        work[i, :size] = unit(size) + bounce
        work[i, size:] = product(bounce, embedded(bounce))

    def double(_, carry):
        for i in range(len(pairs)):
            both = work[i]
            grown = product(both, embedded(both[size:]))
            work[i, :size] = both[:size] + grown[:size]
            work[i, size:] = grown[size:]
        return carry

    if early is not None:
        early()
    lax.fori_loop(0, 2, double, 0)
    if middle is not None:
        middle()
    lax.fori_loop(2, INV_STEPS - 2, double, 0)
    if late is not None:
        late()
    for i, (first, second, emit) in enumerate(pairs):
        partial = work[i, :size]
        resolvent = partial + product(partial, embedded(work[i, size:]))
        second_left = second[LEFT]
        fore = embedded(first[FORE])
        back = embedded(second[BACK])
        leading = product(first[BACK], embedded(resolvent))
        inner = product(resolvent, embedded(second_left))
        emit(LEFT, first[LEFT] + product(leading, embedded(product(second_left, fore))))
        through = product(second[FORE], embedded(first[RIGHT]))
        trailing = second[FORE] + product(through, embedded(inner))
        emit(RIGHT, second[RIGHT] + product(trailing, embedded(product(first[RIGHT], back))))
        emit(BACK, product(leading, back))
        emit(FORE, product(trailing, fore))


def kernel(
    n, levels, sections, probes, prefixes, reflected, transmitted,
    arrived, own, stage, before, work, total, leaving,
    swap_sems, stage_send, stage_recv, pass_send, pass_recv, relay_send, total_sems, out_send, out_recv,
):
    me = lax.axis_index("chain")
    relaying = int(levels >= 3)
    core = me % 2
    sibling = me + 1 - 2 * core
    size = probes.shape[2]

    def partner(stride):
        return me + stride - 2 * stride * ((me // stride) % 2)

    barrier = pltpu.get_barrier_semaphore()
    for level in range(levels + 1):
        pl.semaphore_signal(barrier, inc=1, device_id=(partner(1 << level),), device_id_type=MESH)
    if relaying:
        facing = partner(n // 2) + partner(n // 4) - me
        pl.semaphore_signal(barrier, inc=1, device_id=(facing,), device_id_type=MESH)
    pl.semaphore_wait(barrier, levels + 1 + relaying)

    def remote(source, target, send, recv, device):
        return pltpu.make_async_remote_copy(
            src_ref=source, dst_ref=target, send_sem=send, recv_sem=recv, device_id=(device,), device_id_type=MESH
        )

    swap = remote(sections.at[0, 1 - core], arrived, swap_sems.at[0], swap_sems.at[1], sibling)
    swap.start()

    def joined(block):
        return jnp.concatenate([block[0], block[1]], axis=1)

    vacant = jnp.zeros((size, 2 * size), f32)
    for b in range(4):
        own[core, b] = joined(sections[0, core, b])
        before[b] = vacant if b in (LEFT, RIGHT) else unit(size)
    swap.wait()
    for b in range(4):
        own[1 - core, b] = joined(arrived[b])

    half = size // 2
    side = (me // 2) % 2
    neighbour = partner(2) if levels else me

    def relayed(level):
        return jnp.logical_and(level == levels - 1, relaying == 1)

    def outer(level):
        return jnp.logical_and(relayed(level), (me // (n // 2)) % 2 == (me // max(n // 4, 1)) % 2)

    def place(level, slot, block, part):
        return stage.at[level, slot, block, pl.ds(pl.multiple_of(part * half, half), half)]

    def across(level, stride, block):
        far = partner(stride)
        if relaying:
            far = jnp.where(relayed(level), facing, far)
        part = jnp.where(level == 0, 1 - side, side)
        where = place(level, (me // stride) % 2, block, part)
        return remote(where, where, stage_send.at[level, block], stage_recv.at[level, block], far)

    def across_rest(level, stride, block):
        where = place(level, (me // stride) % 2, block, side)
        return remote(where, where, pass_send.at[level, block], pass_recv.at[level, block], neighbour)

    def passing(level, stride, block):
        where = place(level, 1 - (me // stride) % 2, block, side)
        return remote(where, where, pass_send.at[level, block], pass_recv.at[level, block], neighbour)

    def relay(level, stride, block):
        where = place(level, 1 - (me // stride) % 2, block, side)
        return remote(where, where, relay_send.at[block], stage_recv.at[level, block], partner(n // 4))

    def send(level, stride, block):
        @pl.when(jnp.logical_not(outer(level)))
        def _():
            across(level, stride, block).start()

        @pl.when(level == 0)
        def _():
            across_rest(level, stride, block).start()

    def service(level, stride, block):
        @pl.when(level < levels)
        def _():
            across(level, stride, block).wait_recv()

            @pl.when(level > 0)
            def _():
                passing(level, stride, block).start()

            if relaying:

                @pl.when(jnp.logical_and(relayed(level), jnp.logical_not(outer(level))))
                def _():
                    relay(level, stride, block).start()

    def finish(level, stride, block):
        passing(level, stride, block).wait_recv()

    def needed_first(stride):
        return RIGHT * ((me // stride) % 2)

    def total_copy(k):
        return remote(
            stage.at[levels, 0, (LEFT, FORE)[k]], total.at[k], total_sems.at[0, k], total_sems.at[1, k], sibling
        )

    def emit_stage(level, stride):
        def emit(block, value):
            stage[level, (me // stride) % 2, block] = value

            if block != LEFT:

                @pl.when(level < levels)
                def _():
                    if block == RIGHT:
                        send(level, stride, RIGHT - needed_first(stride))
                        send(level, stride, needed_first(stride))
                    else:
                        send(level, stride, block)

            if block in (LEFT, FORE):

                @pl.when(level == levels)
                def _():
                    total_copy((LEFT, FORE).index(block)).start()

        return emit

    def emit_before(block, value):
        before[block] = value

    if levels:
        first_emit = emit_stage(0, 2)
    else:
        first_emit = emit_stage(0, n)
    star([(own.at[0], own.at[1], first_emit)], work)
    pair_slot = (me // 2) % 2 if levels else 0
    for b in range(4):
        own[1, b] = stage[0, pair_slot, b]

    def climb(level, stride):
        lower, upper = stage.at[level, 0], stage.at[level, 1]

        following, doubled = level + 1, 2 * stride
        finish(level, stride, needed_first(stride))

        def late():
            finish(level, stride, RIGHT - needed_first(stride))
            finish(level, stride, BACK)
            finish(level, stride, FORE)

        star(
            [(lower, upper, emit_stage(following, doubled))], work,
            lambda: service(level, stride, BACK), lambda: service(level, stride, FORE), late,
        )
        first = lambda: service(following, doubled, needed_first(doubled))

        @pl.when((me // stride) % 2 == 1)
        def _():
            star([(lower, before, emit_before)], work, middle=first)

        @pl.when((me // stride) % 2 == 0)
        def _():
            first()

        service(following, doubled, RIGHT - needed_first(doubled))
        return doubled

    if levels:
        service(0, 2, needed_first(2))
        service(0, 2, RIGHT - needed_first(2))
    lax.fori_loop(0, levels, climb, jnp.int32(2))

    def probe(frequency, whole):
        field = embedded(joined(probes[frequency]))
        result = product(whole, field)
        for k, out in enumerate((reflected, transmitted)):
            out[frequency, 0] = result[k * size : (k + 1) * size, :size]
            out[frequency, 1] = result[k * size : (k + 1) * size, size:]

    probe(core, jnp.concatenate([stage[levels, 0, LEFT], stage[levels, 0, FORE]], axis=0))

    def out_copy(block):
        return remote(
            leaving.at[block], prefixes.at[0, core, block], out_send.at[block], out_recv.at[block], sibling
        )

    def emit_away(block, value):
        leaving[block, 0] = value[:, :size]
        leaving[block, 1] = value[:, size:]
        out_copy(block).start()

    def emit_own(block, value):
        prefixes[0, core, block, 0] = value[:, :size]
        prefixes[0, core, block, 1] = value[:, size:]

    star([(before, own.at[1 - core], emit_away), (before, own.at[core], emit_own)], work)

    for k in range(2):
        total_copy(k).wait()
    probe(1 - core, jnp.concatenate([total[0], total[1]], axis=0))

    def drain(level, stride):
        for block in range(4):
            @pl.when(jnp.logical_not(outer(level)))
            def _():
                across(level, stride, block).wait_send()

            passing(level, stride, block).wait_send()
        return 2 * stride

    lax.fori_loop(0, levels, drain, jnp.int32(2))
    if relaying:

        @pl.when(jnp.logical_not(outer(levels - 1)))
        def _():
            for block in range(4):
                relay(levels - 1, n // 2, block).wait_send()

    for block in range(4):
        out_copy(block).wait()


def solution(mesh):
    n = mesh.shape["chain"]
    levels = (n // 2 - 1).bit_length()

    def local(sections, probes):
        size = probes.shape[2]
        wide = (size, 2 * size)
        dma = pltpu.SemaphoreType.DMA
        vmem = pl.BlockSpec(memory_space=pltpu.VMEM)
        return pl.pallas_call(
            functools.partial(kernel, n, levels),
            out_shape=tuple(jax.ShapeDtypeStruct(a.shape, f32) for a in (sections, probes, probes)),
            in_specs=[vmem] * 2,
            out_specs=(vmem,) * 3,
            scratch_shapes=[
                pltpu.VMEM(sections.shape[2:], f32),
                pltpu.VMEM((2, 4) + wide, f32),
                pltpu.VMEM((levels + 1, 2, 4) + wide, f32),
                pltpu.VMEM((4,) + wide, f32),
                pltpu.VMEM((2, 2 * size, 2 * size), f32),
                pltpu.VMEM((2,) + wide, f32),
                pltpu.VMEM(sections.shape[2:], f32),
                dma((2,)),
                dma((max(levels, 1), 4)),
                dma((max(levels, 1), 4)),
                dma((max(levels, 1), 4)),
                dma((max(levels, 1), 4)),
                dma((4,)),
                dma((2, 2)),
                dma((4,)),
                dma((4,)),
            ],
            compiler_params=pltpu.CompilerParams(
                collective_id=0, has_side_effects=True, vmem_limit_bytes=48 * 1024 * 1024
            ),
        )(sections, probes)

    placed = (P("chain", None, None, None, None, None), P(None, None, None, "chain"))
    return jax.shard_map(
        local, mesh=mesh, in_specs=placed, out_specs=(placed[0], placed[1], placed[1]), check_vma=False
    )
```
